32 devices in a mesh: rep: 1, dp: 32 (over x, y, z, core).
Axes of the slice: x: 2, y: 2, z: 4, core: 2. Of those that a mesh axis runs over, the one named last changes fastest.
Arguments:
- g_w_gate: bfloat16 [32, 2, 1024, 2816], P(('rep', 'dp'))
- g_w_up: bfloat16 [32, 2, 1024, 2816], P(('rep', 'dp'))
- g_w_down: bfloat16 [32, 2, 2816, 1024], P(('rep', 'dp'))
- w_gate: bfloat16 [2, 1024, 2816], replicated
- w_up: bfloat16 [2, 1024, 2816], replicated
- w_down: bfloat16 [2, 2816, 1024], replicated
- m_w_gate: float32 [2, 1024, 2816], P(None, 'dp')
- m_w_up: float32 [2, 1024, 2816], P(None, 'dp')
- m_w_down: float32 [2, 2816, 1024], P(None, 'dp')
- v_w_gate: float32 [2, 1024, 2816], P(None, 'dp')
- v_w_up: float32 [2, 1024, 2816], P(None, 'dp')
- v_w_down: float32 [2, 2816, 1024], P(None, 'dp')
Outputs:
- output 1: bfloat16 [2, 1024, 2816], P('rep')
- output 2: bfloat16 [2, 1024, 2816], P('rep')
- output 3: bfloat16 [2, 2816, 1024], P('rep')
- output 4: float32 [2, 1024, 2816], P('rep', 'dp')
- output 5: float32 [2, 1024, 2816], P('rep', 'dp')
- output 6: float32 [2, 2816, 1024], P('rep', 'dp')
- output 7: float32 [2, 1024, 2816], P('rep', 'dp')
- output 8: float32 [2, 1024, 2816], P('rep', 'dp')
- output 9: float32 [2, 2816, 1024], P('rep', 'dp')
All inputs are finite; a program needn't handle non-finite values.
Results may differ from the reference program's by a relative error of at most 0.022.
Values are sent between devices in bfloat16 or wider.
A program may use at most 2 GiB of HBM per device.

```python
import jax
import jax.numpy as jnp
from jax import lax

DEVICES = 32
D = 1024
FF = 2816
LAYERS = 2
NAMES = ("w_gate", "w_up", "w_down")
SHAPES = {"w_gate": (LAYERS, D, FF), "w_up": (LAYERS, D, FF), "w_down": (LAYERS, FF, D)}


def setup_inputs(seed: int = 0, part: int = 0) -> dict:
    kz, *keys = jax.random.split(jax.random.key(seed), 1 + 5 * len(NAMES))
    loud = 2.0 ** jax.random.uniform(kz, (), jnp.float32, -1.0, 1.0)
    drawn = {}
    for name, key, both in zip(NAMES, keys[:3], keys[3:6], strict=True):
        own = jax.random.normal(jax.random.fold_in(key, part), (DEVICES, *SHAPES[name]), jnp.float32)
        shared = jax.random.normal(jax.random.fold_in(both, part), SHAPES[name], jnp.float32)
        drawn["g_" + name] = (loud * (0.7 * shared / DEVICES + 0.7 * own * DEVICES**-0.5)).astype(jnp.bfloat16)
    for name, key in zip(NAMES, keys[6:9], strict=True):
        drawn[name] = (jax.random.normal(key, SHAPES[name], jnp.float32) * SHAPES[name][1] ** -0.5).astype(jnp.bfloat16)
    for name, key in zip(NAMES, keys[9:12], strict=True):
        drawn["m_" + name] = loud * 0.5 * jax.random.normal(key, SHAPES[name], jnp.float32)
    for name, key in zip(NAMES, keys[12:15], strict=True):
        drawn["v_" + name] = loud * loud * jax.random.uniform(key, SHAPES[name], jnp.float32, 0.5, 1.5)
    return drawn


def adamw(w, m, v, g):
    m = 0.9 * m + 0.1 * g
    v = 0.95 * v + 0.05 * g * g
    step = m * lax.rsqrt(v + 1e-8) + 0.1 * w
    return (w - 0.02 * step).astype(jnp.bfloat16), m, v


def reference(g_w_gate, g_w_up, g_w_down, w_gate, w_up, w_down, m_w_gate, m_w_up, m_w_down, v_w_gate, v_w_up, v_w_down):
    def total(terms):
        return lax.scan(lambda so_far, term: (so_far + term.astype(jnp.float32), None), jnp.zeros(terms.shape[1:], jnp.float32), terms)[0]

    gradients = [total(terms).astype(jnp.bfloat16).astype(jnp.float32) for terms in (g_w_gate, g_w_up, g_w_down)]
    new = [
        adamw(w.astype(jnp.float32), m, v, g)
        for w, m, v, g in zip((w_gate, w_up, w_down), (m_w_gate, m_w_up, m_w_down), (v_w_gate, v_w_up, v_w_down), gradients, strict=True)
    ]
    return tuple(one[which] for which in range(3) for one in new)
```

```python
import functools

import jax
import jax.numpy as jnp
from jax import lax
from jax.experimental import pallas as pl
from jax.experimental.pallas import tpu as pltpu
from jax.sharding import PartitionSpec as P

MESH = pl.DeviceIdType.MESH
F32, BF16 = jnp.float32, jnp.bfloat16
SPLIT = (128, 128, 96)
HALVES = 2
S1, S2, ZU, ZD, GU, GD, G1, G2, GP = 0, 1, 2, 5, 8, 11, 14, 15, 16
KINDS = 17


def adamw(w, m, v, g):
    m = 0.9 * m + 0.1 * g
    v = 0.95 * v + 0.05 * g * g
    step = m * lax.rsqrt(v + 1e-8) + 0.1 * w
    return (w - 0.02 * step).astype(BF16), m, v


def kernel(split, mats, *refs):
    (g0, g1, g2, w0, w1, w2, m0, m1, m2, v0, v1, v2, out, mo0, mo1, mo2, vo0, vo1, vo2, *scratch) = refs
    own, peer, wb, mb, vb, r1x, r2x, zux, zdx, r1y, r2y, zuy, zdy, r1z, r2z, zuz, zdz, *sems = scratch
    rsem, ssem, lsem, osem, psem, pssem, isem, esem = sems
    units = mats * HALVES
    row = (0, split[0], split[0] + split[1])
    rows = [pl.ds(row[k], split[k]) for k in range(3)]

    me = lax.axis_index("dp")
    c, z, y, x = me % 2, (me // 2) % 4, (me // 8) % 2, me // 16

    def at(x, y, z, c):
        return (0, ((x * 2 + y) * 4 + z) * 2 + c)

    xn, yn, zu, zd, cn = at(1 - x, y, z, c), at(x, 1 - y, z, c), at(x, y, z + 1, c), at(x, y, z - 1, c), at(x, y, z, 1 - c)

    def send(src, dst, k, kind, u, to, land=None):
        pltpu.make_async_remote_copy(
            src_ref=src,
            dst_ref=dst,
            send_sem=ssem.at[k, kind],
            recv_sem=rsem.at[k, kind if land is None else land, u],
            device_id=to,
            device_id_type=MESH,
        ).start()

    def landed(ref, sem):
        pltpu.make_async_copy(ref, ref, sem).wait()

    @pl.when(z == 0)
    def _():
        for ref in (zux, zuy, zuz):
            for u in range(units):
                ref[u] = jnp.zeros(ref.shape[1:], BF16)

    @pl.when(z == 3)
    def _():
        for ref in (zdx, zdy, zdz):
            for u in range(units):
                ref[u] = jnp.zeros(ref.shape[1:], BF16)

    barrier = pltpu.get_barrier_semaphore()
    for to in (xn, yn, cn):
        pl.semaphore_signal(barrier, inc=1, device_id=to, device_id_type=MESH)

    @pl.when(z < 3)
    def _():
        pl.semaphore_signal(barrier, inc=1, device_id=zu, device_id_type=MESH)

    @pl.when(z > 0)
    def _():
        pl.semaphore_signal(barrier, inc=1, device_id=zd, device_id_type=MESH)

    pl.semaphore_wait(barrier, 3 + jnp.where(z > 0, 1, 0) + jnp.where(z < 3, 1, 0))

    for u in range(units):
        mat, h = u // HALVES, u % HALVES
        g = (g0, g1, g2)[mat // 2]
        pltpu.make_async_remote_copy(
            src_ref=g.at[mat % 2, :, :, :, 1 - c, h],
            dst_ref=peer.at[u],
            send_sem=pssem.at[0],
            recv_sem=psem.at[u],
            device_id=cn,
            device_id_type=MESH,
        ).start()
        pltpu.make_async_copy(g.at[mat % 2, :, :, :, c, h], own.at[u], osem.at[u]).start()
    incoming = []
    for a in range(mats // 2):
        two = pl.ds(2 * a, 2)
        incoming.append(pltpu.make_async_copy((w0, w1, w2)[a].at[:, me], wb.at[two], isem.at[a]))
        incoming.append(pltpu.make_async_copy((m0, m1, m2)[a], mb.at[two], isem.at[3 + a]))
        incoming.append(pltpu.make_async_copy((v0, v1, v2)[a], vb.at[two], isem.at[6 + a]))
    for copy in incoming:
        copy.start()

    def total(terms):
        acc = terms[0].astype(F32)
        for term in terms[1:]:
            acc = acc + term.astype(F32)
        return acc

    def loop(n, body):
        lax.fori_loop(0, n, lambda i, _: (body(i), 0)[1], 0)

    def first_colours(k):
        f, s, fn, sn = ((x, y, xn, yn), (y, x, yn, xn))[k]
        r1, r2, up, down = ((r1x, r2x, zux, zdx), (r1y, r2y, zuy, zdy))[k]
        n = rows[k]

        def xy(one, two):
            return (one, two) if k == 0 else (two, one)

        def base(u, zj):
            i = (u, x, y, zj, n)
            return [own[i], peer[i], r1[u, s, zj], r2[u, zj]]

        def a(u):
            def body(i):
                j = (u, *xy(1 - f, i // 4), i % 4, n)
                own[j] = total([own[j], peer[j]]).astype(BF16)

            loop(8, body)
            send(own.at[(u, *xy(1 - f, slice(None)), slice(None), n)], r1.at[u], k, S1, u, fn)

        def b(u):
            landed(r1.at[u], rsem.at[k, S1, u])

            def body(i):
                j = (u, *xy(f, 1 - s), i, n)
                own[j] = total([own[j], peer[j], r1[u, 1 - s, i]]).astype(BF16)

            loop(4, body)
            send(own.at[(u, *xy(f, 1 - s), slice(None), n)], r2.at[u], k, S2, u, sn)

        def hop(u, d):
            if d == 3:
                landed(r2.at[u], rsem.at[k, S2, u])

            @pl.when(z + d <= 3)
            def _():
                if d < 3:
                    pl.when(z > 0)(lambda: landed(up.at[u, d], rsem.at[k, ZU + d, u]))
                i = (u, x, y, z + d, n)
                own[i] = total(base(u, z + d) + ([up[u, d]] if d < 3 else [])).astype(BF16)
                send(own.at[i], up.at[u, d - 1], k, ZU + d - 1, u, zu)

            @pl.when(z - d >= 0)
            def _():
                if d < 3:
                    pl.when(z < 3)(lambda: landed(down.at[u, d], rsem.at[k, ZD + d, u]))
                i = (u, x, y, z - d, n)
                own[i] = total(base(u, z - d) + ([down[u, d]] if d < 3 else [])).astype(BF16)
                send(own.at[i], down.at[u, d - 1], k, ZD + d - 1, u, zd)

        def update(u):
            mat, h = u // HALVES, u % HALVES
            pl.when(z > 0)(lambda: landed(up.at[u, 0], rsem.at[k, ZU, u]))
            pl.when(z < 3)(lambda: landed(down.at[u, 0], rsem.at[k, ZD, u]))

            def body(i):
                p, q = pl.ds(row[k] + i * 16, 16), pl.ds(i * 16, 16)
                j = (u, x, y, z, p)
                g = total([own[j], peer[j], r1[u, s, z, q], r2[u, z, q], up[u, 0, q], down[u, 0, q]]).astype(BF16).astype(F32)
                j = (mat, h, p)
                wb[j], mb[j], vb[j] = adamw(wb[j].astype(F32), mb[j], vb[j], g)

            loop(split[k] // 16, body)
            mine = out.at[mat, x, y, z, c, h, n]
            pltpu.make_async_copy(wb.at[mat, h, n], mine, lsem.at[k, u]).start()
            pl.when(z < 3)(lambda: send(wb.at[mat, h, n], mine, k, GU, u, zu))
            pl.when(z > 0)(lambda: send(wb.at[mat, h, n], mine, k, GD, u, zd))

        def forward(u, d):
            mat, h = u // HALVES, u % HALVES

            @pl.when(z - d >= 0)
            def _():
                ref = out.at[mat, x, y, z - d, c, h, n]
                landed(ref, rsem.at[k, GU + d - 1, u])
                if d < 3:
                    pl.when(z < 3)(lambda: send(ref, ref, k, GU + d, u, zu))

            @pl.when(z + d <= 3)
            def _():
                ref = out.at[mat, x, y, z + d, c, h, n]
                landed(ref, rsem.at[k, GD + d - 1, u])
                if d < 3:
                    pl.when(z > 0)(lambda: send(ref, ref, k, GD + d, u, zd))

        def second(u):
            mat, h = u // HALVES, u % HALVES
            landed(out.at[mat, x, y, z, c, h, n], lsem.at[k, u])
            ref = out.at[mat, x, y, :, c, h, n]
            send(ref, ref, k, G1, u, sn)

        def third(u):
            mat, h = u // HALVES, u % HALVES
            landed(out.at[(mat, *xy(f, 1 - s), slice(None), c, h, n)], rsem.at[k, G1, u])
            ref = out.at[(mat, *xy(f, slice(None)), slice(None), c, h, n)]
            send(ref, ref, k, G2, u, fn)

        def last(u):
            mat, h = u // HALVES, u % HALVES
            landed(out.at[(mat, *xy(1 - f, slice(None)), slice(None), c, h, n)], rsem.at[k, G2, u])
            ref = out.at[mat, :, :, :, c, h, n]
            send(ref, ref, k, GP, u, cn)

        def drain():
            landed(own.at[(slice(None), *xy(1 - f, slice(None)), slice(None), n)], ssem.at[k, S1])
            landed(own.at[(slice(None), *xy(f, 1 - s), slice(None), n)], ssem.at[k, S2])
            for d in (1, 2, 3):
                pl.when(z + d <= 3)(lambda: landed(own.at[:, x, y, z + d, n], ssem.at[k, ZU + d - 1]))
                pl.when(z - d >= 0)(lambda: landed(own.at[:, x, y, z - d, n], ssem.at[k, ZD + d - 1]))
            for d in (0, 1, 2):
                pl.when((z - d >= 0) & (z < 3))(lambda: landed(out.at[:, x, y, z - d, c, :, n], ssem.at[k, GU + d]))
                pl.when((z + d <= 3) & (z > 0))(lambda: landed(out.at[:, x, y, z + d, c, :, n], ssem.at[k, GD + d]))
            landed(out.at[:, x, y, :, c, :, n], ssem.at[k, G1])
            landed(out.at[(slice(None), *xy(f, slice(None)), slice(None), c, slice(None), n)], ssem.at[k, G2])

        return a, b, hop, update, forward, second, third, last, drain

    def z_colour():
        k, n = 2, rows[2]

        def hop(u, d):
            def side(sign, ref, kind, to):
                zj = z + sign * d
                if d < 3:
                    pl.when(z > 0 if sign > 0 else z < 3)(lambda: landed(ref.at[u, d], rsem.at[k, kind + d, u]))

                def body(i):
                    j = (u, i // 2, i % 2, zj, n)
                    own[j] = total([own[j], peer[j]] + ([ref[u, d, i // 2, i % 2]] if d < 3 else [])).astype(BF16)

                loop(4, body)
                send(own.at[u, :, :, zj, n], ref.at[u, d - 1], k, kind + d - 1, u, to)

            pl.when(z + d <= 3)(lambda: side(1, zuz, ZU, zu))
            pl.when(z - d >= 0)(lambda: side(-1, zdz, ZD, zd))

        def base(u, xj, yj):
            i = (u, xj, yj, z, n)
            return [own[i], peer[i], zuz[u, 0, xj, yj], zdz[u, 0, xj, yj]]

        def to_x(u):
            pl.when(z > 0)(lambda: landed(zuz.at[u, 0], rsem.at[k, ZU, u]))
            pl.when(z < 3)(lambda: landed(zdz.at[u, 0], rsem.at[k, ZD, u]))

            def body(i):
                own[u, 1 - x, i, z, n] = total(base(u, 1 - x, i)).astype(BF16)

            loop(2, body)
            send(own.at[u, 1 - x, :, z, n], r1z.at[u], k, S1, u, xn)

        def to_y(u):
            landed(r1z.at[u], rsem.at[k, S1, u])
            i = (u, x, 1 - y, z, n)
            own[i] = total(base(u, x, 1 - y) + [r1z[u, 1 - y]]).astype(BF16)
            send(own.at[i], r2z.at[u], k, S2, u, yn)

        def update(u):
            mat, h = u // HALVES, u % HALVES
            landed(r2z.at[u], rsem.at[k, S2, u])

            def body(i):
                p, q = pl.ds(row[k] + i * 16, 16), pl.ds(i * 16, 16)
                j = (u, x, y, z, p)
                g = total([own[j], peer[j], zuz[u, 0, x, y, q], zdz[u, 0, x, y, q], r1z[u, y, q], r2z[u, q]]).astype(BF16).astype(F32)
                j = (mat, h, p)
                wb[j], mb[j], vb[j] = adamw(wb[j].astype(F32), mb[j], vb[j], g)

            loop(split[k] // 16, body)
            mine = out.at[mat, x, y, z, c, h, n]
            pltpu.make_async_copy(wb.at[mat, h, n], mine, lsem.at[k, u]).start()
            send(wb.at[mat, h, n], mine, k, G1, u, yn)

        def second(u):
            mat, h = u // HALVES, u % HALVES
            landed(out.at[mat, x, y, z, c, h, n], lsem.at[k, u])
            landed(out.at[mat, x, 1 - y, z, c, h, n], rsem.at[k, G1, u])
            ref = out.at[mat, x, :, z, c, h, n]
            send(ref, ref, k, G2, u, xn)

        def third(u):
            mat, h = u // HALVES, u % HALVES
            landed(out.at[mat, 1 - x, :, z, c, h, n], rsem.at[k, G2, u])
            ref = out.at[mat, :, :, z, c, h, n]
            pl.when(z < 3)(lambda: send(ref, ref, k, GU, u, zu))
            pl.when(z > 0)(lambda: send(ref, ref, k, GD, u, zd))

        def forward(u, d):
            mat, h = u // HALVES, u % HALVES

            @pl.when(z - d >= 0)
            def _():
                ref = out.at[mat, :, :, z - d, c, h, n]
                landed(ref, rsem.at[k, GU + d - 1, u])
                if d < 3:
                    pl.when(z < 3)(lambda: send(ref, ref, k, GU + d, u, zu))

            @pl.when(z + d <= 3)
            def _():
                ref = out.at[mat, :, :, z + d, c, h, n]
                landed(ref, rsem.at[k, GD + d - 1, u])
                if d < 3:
                    pl.when(z > 0)(lambda: send(ref, ref, k, GD + d, u, zd))

        def last(u):
            mat, h = u // HALVES, u % HALVES
            ref = out.at[mat, :, :, :, c, h, n]
            send(ref, ref, k, GP, u, cn)

        def drain():
            for d in (1, 2, 3):
                pl.when(z + d <= 3)(lambda: landed(own.at[:, :, :, z + d, n], ssem.at[k, ZU + d - 1]))
                pl.when(z - d >= 0)(lambda: landed(own.at[:, :, :, z - d, n], ssem.at[k, ZD + d - 1]))
            landed(own.at[:, 1 - x, :, z, n], ssem.at[k, S1])
            landed(own.at[:, x, 1 - y, z, n], ssem.at[k, S2])
            landed(out.at[:, x, y, z, c, :, n], ssem.at[k, G1])
            landed(out.at[:, x, :, z, c, :, n], ssem.at[k, G2])
            for d in (0, 1, 2):
                pl.when((z - d >= 0) & (z < 3))(lambda: landed(out.at[:, :, :, z - d, c, :, n], ssem.at[k, GU + d]))
                pl.when((z + d <= 3) & (z > 0))(lambda: landed(out.at[:, :, :, z + d, c, :, n], ssem.at[k, GD + d]))

        return hop, to_x, to_y, update, second, third, forward, last, drain

    xa, xb, xhop, xupdate, xforward, xsecond, xthird, xlast, xdrain = first_colours(0)
    ya, yb, yhop, yupdate, yforward, ysecond, ythird, ylast, ydrain = first_colours(1)
    zhop, zx, zy, zupdate, zsecond, zthird, zforward, zlast, zdrain = z_colour()

    def arrive(u):
        landed(peer.at[u], psem.at[u])
        landed(own.at[u], osem.at[u])

    def moments(u):
        for a in range(mats // 2):

            @pl.when(u == 2 * HALVES * (a + 1) - 1)
            def _():
                two = pl.ds(2 * a, 2)
                pltpu.make_async_copy(mb.at[two], (mo0, mo1, mo2)[a], esem.at[a]).start()
                pltpu.make_async_copy(vb.at[two], (vo0, vo1, vo2)[a], esem.at[3 + a]).start()

    def settle(u):
        for a in range(mats // 2):

            @pl.when(u == 2 * HALVES * a)
            def _():
                for copy in incoming[3 * a : 3 * a + 3]:
                    copy.wait()

    plan = [
        (0, arrive),
        (0, xa),
        (0, ya),
        (0, lambda u: zhop(u, 3)),
        (1, xb),
        (1, yb),
        (0, lambda u: zhop(u, 2)),
        (2, lambda u: xhop(u, 3)),
        (2, lambda u: yhop(u, 3)),
        (2, zx),
        (3, zy),
        (1, lambda u: zhop(u, 1)),
        (2, lambda u: xhop(u, 2)),
        (2, lambda u: yhop(u, 2)),
        (5, zsecond),
        (4, lambda u: xforward(u, 1)),
        (4, lambda u: yforward(u, 1)),
        (6, zthird),
        (5, (lambda u: xforward(u, 3), xsecond)),
        (5, (lambda u: yforward(u, 3), ysecond)),
        (2, lambda u: xhop(u, 1)),
        (2, lambda u: yhop(u, 1)),
        (7, lambda u: zforward(u, 1)),
        (6, xthird),
        (6, ythird),
        (4, lambda u: xforward(u, 2)),
        (4, lambda u: yforward(u, 2)),
        (7, lambda u: zforward(u, 2)),
        (3, settle),
        (3, xupdate),
        (3, yupdate),
        (4, zupdate),
        (4, moments),
        (7, xlast),
        (7, ylast),
        (8, (lambda u: zforward(u, 3), zlast)),
    ]

    def run(stages, u):
        for stage in stages if isinstance(stages, tuple) else (stages,):
            stage(u)

    @pl.loop(0, units + max(lag for lag, _ in plan))
    def _(t):
        for lag, stage in plan:
            u = t - lag
            pl.when((u >= 0) & (u < units))(functools.partial(run, stage, u))

    for k in range(3):

        @pl.loop(0, units)
        def _(u):
            landed(out.at[u // HALVES, :, :, :, 1 - c, u % HALVES, rows[k]], rsem.at[k, GP, u])

        landed(out.at[:, :, :, :, c, :, rows[k]], ssem.at[k, GP])
    for a in range(mats // 2):
        two = pl.ds(2 * a, 2)
        landed(mb.at[two], esem.at[a])
        landed(vb.at[two], esem.at[3 + a])
    landed(peer, pssem.at[0])
    xdrain()
    ydrain()
    zdrain()


def call(terms, weights, m, v, split=SPLIT):
    mats, high = 2 * len(terms), sum(split)
    units = mats * HALVES
    rx, ry, rz = split
    some = jax.ShapeDtypeStruct
    moment = some((2, HALVES, high, 128), F32)
    block = [
        pltpu.VMEM((units, 2, 2, 4, high, 128), BF16),
        pltpu.VMEM((units, 2, 2, 4, high, 128), BF16),
        pltpu.VMEM((mats, HALVES, high, 128), BF16),
        pltpu.VMEM((mats, HALVES, high, 128), F32),
        pltpu.VMEM((mats, HALVES, high, 128), F32),
    ]
    for r in (rx, ry):
        block += [
            pltpu.VMEM((units, 2, 4, r, 128), BF16),
            pltpu.VMEM((units, 4, r, 128), BF16),
            pltpu.VMEM((units, 3, r, 128), BF16),
            pltpu.VMEM((units, 3, r, 128), BF16),
        ]
    block += [
        pltpu.VMEM((units, 2, rz, 128), BF16),
        pltpu.VMEM((units, rz, 128), BF16),
        pltpu.VMEM((units, 3, 2, 2, rz, 128), BF16),
        pltpu.VMEM((units, 3, 2, 2, rz, 128), BF16),
    ]
    dma = pltpu.SemaphoreType.DMA
    return pl.pallas_call(
        functools.partial(kernel, split, mats),
        out_shape=[some((mats, 2, 2, 4, 2, HALVES, high, 128), BF16)] + [moment] * 6,
        in_specs=[pl.BlockSpec(memory_space=pl.ANY)] * 12,
        out_specs=[pl.BlockSpec(memory_space=pl.ANY)] * 7,
        scratch_shapes=block
        + [dma((3, KINDS, units)), dma((3, KINDS)), dma((3, units)), dma((units,)), dma((units,)), dma((1,)), dma((9,)), dma((6,))],
        compiler_params=pltpu.CompilerParams(collective_id=0, has_side_effects=True, vmem_limit_bytes=67043328),
        name="step",
    )(*terms, *weights, *m, *v)


def tiles(a):
    *lead, rows, columns = a.shape
    a = a.reshape(*lead, rows // 8, 8, columns // 128, 128)
    return jnp.swapaxes(a, -3, -2).reshape(*lead, rows * columns // 128, 128)


def untiles(a, rows, columns):
    lead = a.shape[:-2]
    a = a.reshape(*lead, rows // 8, columns // 128, 8, 128)
    return jnp.swapaxes(a, -3, -2).reshape(*lead, rows, columns)


def solution(mesh):
    def step(*arrays):
        terms, weights, m, v = (arrays[i : i + 3] for i in (0, 3, 6, 9))
        high = sum(SPLIT)
        out = call(
            [tiles(t[0]).reshape(2, 2, 2, 4, 2, HALVES, high, 128) for t in terms],
            [tiles(w).reshape(2, 32, HALVES, high, 128) for w in weights],
            [tiles(one).reshape(2, HALVES, high, 128) for one in m],
            [tiles(one).reshape(2, HALVES, high, 128) for one in v],
        )
        whole = [untiles(out[0][2 * i : 2 * i + 2].reshape(2, -1, 128), *w.shape[1:]) for i, w in enumerate(weights)]
        moments = [untiles(one.reshape(2, -1, 128), *old.shape[1:]) for one, old in zip(out[1:], (*m, *v), strict=True)]
        return (*whole, *moments)

    all_of, cut = P(None, None, None), P(None, "dp", None)
    return jax.shard_map(
        step,
        mesh=mesh,
        in_specs=(P(("rep", "dp"), None, None, None),) * 3 + (all_of,) * 3 + (cut,) * 6,
        out_specs=(P("rep", None, None),) * 3 + (P("rep", "dp", None),) * 6,
        check_vma=False,
    )
```

```python
import functools
import math

import jax
import jax.numpy as jnp
from jax import lax
from jax.experimental import pallas as pl
from jax.experimental.pallas import tpu as pltpu
from jax.sharding import PartitionSpec as P

MESH = pl.DeviceIdType.MESH
F32, BF16 = jnp.float32, jnp.bfloat16
SPLIT = (128, 128, 96)
HALVES = 2
PLAN = (
    (0, "arrive", 0),
    (9, "f2", 2),
    (5, "free", 2),
    (1, "b", 1),
    (4, "free", 1),
    (0, "a", 1),
    (4, "go", 0),
    (4, "go", 1),
    (10, "f3", 2),
    (0, "a", 0),
    (3, "h1", 1),
    (6, "s", 2),
    (7, "t", 2),
    (0, "h3", 2),
    (8, "t", 0),
    (3, "b", 2),
    (8, "l", 1),
    (3, "h1", 0),
    (5, "f3", 0),
    (2, "h3", 0),
    (5, "f3", 1),
    (4, "f1", 0),
    (5, "go", 2),
    (4, "f1", 1),
    (1, "b", 0),
    (10, "l", 2),
    (5, "s", 1),
    (1, "h1", 2),
    (6, "s", 0),
    (6, "t", 1),
    (4, "f2", 0),
    (7, "f1", 2),
    (4, "up", 2),
    (2, "a", 2),
    (0, "h2", 2),
    (3, "up", 0),
    (3, "free", 0),
    (3, "up", 1),
    (1, "h3", 1),
    (4, "f2", 1),
    (2, "h2", 1),
    (11, "l", 0),
    (2, "h2", 0),
)
S1, S2, ZU, ZD, GU, GD, G1, G2, GP = 0, 1, 2, 5, 8, 11, 14, 15, 16
SCATTER, KINDS = 8, 17
X, Y, UP, DOWN, CORE = range(5)


def adamw(w, m, v, g):
    m = 0.9 * m + 0.1 * g
    v = 0.95 * v + 0.05 * g * g
    step = m * lax.rsqrt(v + 1e-8) + 0.1 * w
    return (w - 0.02 * step).astype(BF16), m, v


def kernel(split, mats, *refs):
    (g0, g1, g2, w0, w1, w2, m0, m1, m2, v0, v1, v2, own, peer, mb, vb, *scratch) = refs
    wb, r1x, r2x, zux, zdx, r1y, r2y, zuy, zdy, r1z, r2z, zuz, zdz, *sems = scratch
    rsem, ssem, gsem, osem, psem, pssem, isem, credit = sems
    units = mats * HALVES
    row = (0, split[0], split[0] + split[1])
    rows = [pl.ds(row[k], split[k]) for k in range(3)]

    me = lax.axis_index("dp")
    c, z, y, x = me % 2, (me // 2) % 4, (me // 8) % 2, me // 16

    def at(x, y, z, c):
        return (0, ((x * 2 + y) * 4 + z) * 2 + c)

    xn, yn, zu, zd, cn = at(1 - x, y, z, c), at(x, 1 - y, z, c), at(x, y, z + 1, c), at(x, y, z - 1, c), at(x, y, z, 1 - c)

    def send(src, dst, k, kind, u, to, land=None):
        pltpu.make_async_remote_copy(
            src_ref=src,
            dst_ref=dst,
            send_sem=ssem.at[k, kind, u] if kind < SCATTER else gsem.at[k, kind - SCATTER],
            recv_sem=rsem.at[k, kind if land is None else land, u],
            device_id=to,
            device_id_type=MESH,
        ).start()

    def landed(ref, sem):
        pltpu.make_async_copy(ref, ref, sem).wait()

    def give(k):
        for side, to in ((X, xn), (Y, yn), (CORE, cn)):
            pl.semaphore_signal(credit.at[k, side], inc=1, device_id=to, device_id_type=MESH)
        pl.when(z < 3)(lambda: pl.semaphore_signal(credit.at[k, DOWN], inc=1, device_id=zu, device_id_type=MESH))
        pl.when(z > 0)(lambda: pl.semaphore_signal(credit.at[k, UP], inc=1, device_id=zd, device_id_type=MESH))

    def take(k, side):
        pl.semaphore_wait(credit.at[k, side], 1)

    @pl.when(z == 0)
    def _():
        for ref in (zux, zuy, zuz):
            for u in range(units):
                ref[u] = jnp.zeros(ref.shape[1:], BF16)

    @pl.when(z == 3)
    def _():
        for ref in (zdx, zdy, zdz):
            for u in range(units):
                ref[u] = jnp.zeros(ref.shape[1:], BF16)

    barrier = pltpu.get_barrier_semaphore()
    for to in (xn, yn, cn):
        pl.semaphore_signal(barrier, inc=1, device_id=to, device_id_type=MESH)

    @pl.when(z < 3)
    def _():
        pl.semaphore_signal(barrier, inc=1, device_id=zu, device_id_type=MESH)

    @pl.when(z > 0)
    def _():
        pl.semaphore_signal(barrier, inc=1, device_id=zd, device_id_type=MESH)

    pl.semaphore_wait(barrier, 3 + jnp.where(z > 0, 1, 0) + jnp.where(z < 3, 1, 0))

    for u in range(units):
        mat, h = u // HALVES, u % HALVES
        g = (g0, g1, g2)[mat // 2]
        pltpu.make_async_remote_copy(
            src_ref=g.at[mat % 2, :, :, :, 1 - c, h],
            dst_ref=peer.at[u],
            send_sem=pssem.at[0],
            recv_sem=psem.at[u],
            device_id=cn,
            device_id_type=MESH,
        ).start()
        pltpu.make_async_copy(g.at[mat % 2, :, :, :, c, h], own.at[u], osem.at[u]).start()
    incoming = []
    for a in range(mats // 2):
        two = pl.ds(2 * a, 2)
        incoming.append(pltpu.make_async_copy((w0, w1, w2)[a].at[:, me], wb.at[two], isem.at[a]))
        incoming.append(pltpu.make_async_copy((m0, m1, m2)[a], mb.at[two], isem.at[3 + a]))
        incoming.append(pltpu.make_async_copy((v0, v1, v2)[a], vb.at[two], isem.at[6 + a]))
    for copy in incoming:
        copy.start()

    def total(terms):
        acc = terms[0].astype(F32)
        for term in terms[1:]:
            acc = acc + term.astype(F32)
        return acc

    def loop(n, body):
        lax.fori_loop(0, n, lambda i, _: (body(i), 0)[1], 0)

    def hops(hop, forward):
        scatter = {f"h{d}": functools.partial(hop, d=d) for d in (1, 2, 3)}
        return scatter | {f"f{d}": functools.partial(forward, d=d) for d in (1, 2, 3)}

    def first_colours(k):
        f, s, fn, sn = ((x, y, xn, yn), (y, x, yn, xn))[k]
        first_side, second_side = ((X, Y), (Y, X))[k]
        r1, r2, up, down = ((r1x, r2x, zux, zdx), (r1y, r2y, zuy, zdy))[k]
        n = rows[k]

        def xy(one, two):
            return (one, two) if k == 0 else (two, one)

        def base(u, zj):
            i = (u, x, y, zj, n)
            return [own[i], peer[i], r1[u, s, zj], r2[u, zj]]

        def a(u):
            def body(i):
                j = (u, *xy(1 - f, i // 4), i % 4, n)
                own[j] = total([own[j], peer[j]]).astype(BF16)

            loop(8, body)
            send(own.at[(u, *xy(1 - f, slice(None)), slice(None), n)], r1.at[u], k, S1, u, fn)

        def b(u):
            landed(r1.at[u], rsem.at[k, S1, u])

            def body(i):
                j = (u, *xy(f, 1 - s), i, n)
                own[j] = total([own[j], peer[j], r1[u, 1 - s, i]]).astype(BF16)

            loop(4, body)
            send(own.at[(u, *xy(f, 1 - s), slice(None), n)], r2.at[u], k, S2, u, sn)

        def hop(u, d):
            if d == 3:
                landed(r2.at[u], rsem.at[k, S2, u])

            @pl.when(z + d <= 3)
            def _():
                if d < 3:
                    pl.when(z > 0)(lambda: landed(up.at[u, d], rsem.at[k, ZU + d, u]))
                i = (u, x, y, z + d, n)
                own[i] = total(base(u, z + d) + ([up[u, d]] if d < 3 else [])).astype(BF16)
                send(own.at[i], up.at[u, d - 1], k, ZU + d - 1, u, zu)

            @pl.when(z - d >= 0)
            def _():
                if d < 3:
                    pl.when(z < 3)(lambda: landed(down.at[u, d], rsem.at[k, ZD + d, u]))
                i = (u, x, y, z - d, n)
                own[i] = total(base(u, z - d) + ([down[u, d]] if d < 3 else [])).astype(BF16)
                send(own.at[i], down.at[u, d - 1], k, ZD + d - 1, u, zd)

        def update(u):
            mat, h = u // HALVES, u % HALVES
            pl.when(z > 0)(lambda: landed(up.at[u, 0], rsem.at[k, ZU, u]))
            pl.when(z < 3)(lambda: landed(down.at[u, 0], rsem.at[k, ZD, u]))

            def body(i):
                p, q = pl.ds(row[k] + i * 16, 16), pl.ds(i * 16, 16)
                j = (u, x, y, z, p)
                g = total([own[j], peer[j], r1[u, s, z, q], r2[u, z, q], up[u, 0, q], down[u, 0, q]]).astype(BF16).astype(F32)
                i = (mat, h, p)
                own[j], mb[i], vb[i] = adamw(wb[i].astype(F32), mb[i], vb[i], g)

            loop(split[k] // 16, body)

        def free(u):
            landed(own.at[(u, *xy(1 - f, slice(None)), slice(None), n)], ssem.at[k, S1, u])
            landed(own.at[(u, *xy(f, 1 - s), slice(None), n)], ssem.at[k, S2, u])
            for d in (1, 2, 3):
                pl.when(z + d <= 3)(lambda: landed(own.at[u, x, y, z + d, n], ssem.at[k, ZU + d - 1, u]))
                pl.when(z - d >= 0)(lambda: landed(own.at[u, x, y, z - d, n], ssem.at[k, ZD + d - 1, u]))
            give(k)

        def go(u):
            mine = own.at[u, x, y, z, n]

            @pl.when(z < 3)
            def _():
                take(k, UP)
                send(mine, mine, k, GU, u, zu)

            @pl.when(z > 0)
            def _():
                take(k, DOWN)
                send(mine, mine, k, GD, u, zd)

        def forward(u, d):

            @pl.when(z - d >= 0)
            def _():
                ref = own.at[u, x, y, z - d, n]
                landed(ref, rsem.at[k, GU + d - 1, u])
                if d < 3:
                    pl.when(z < 3)(lambda: send(ref, ref, k, GU + d, u, zu))

            @pl.when(z + d <= 3)
            def _():
                ref = own.at[u, x, y, z + d, n]
                landed(ref, rsem.at[k, GD + d - 1, u])
                if d < 3:
                    pl.when(z > 0)(lambda: send(ref, ref, k, GD + d, u, zd))

        def second(u):
            ref = own.at[u, x, y, :, n]
            take(k, second_side)
            send(ref, ref, k, G1, u, sn)

        def third(u):
            landed(own.at[(u, *xy(f, 1 - s), slice(None), n)], rsem.at[k, G1, u])
            ref = own.at[(u, *xy(f, slice(None)), slice(None), n)]
            take(k, first_side)
            send(ref, ref, k, G2, u, fn)

        def last(u):
            landed(own.at[(u, *xy(1 - f, slice(None)), slice(None), n)], rsem.at[k, G2, u])
            ref = own.at[u, :, :, :, n]
            take(k, CORE)
            send(ref, peer.at[u, :, :, :, n], k, GP, u, cn)

        def drain():
            for d in (0, 1, 2):
                pl.when((z - d >= 0) & (z < 3))(lambda: landed(own.at[:, x, y, z - d, n], gsem.at[k, GU + d - SCATTER]))
                pl.when((z + d <= 3) & (z > 0))(lambda: landed(own.at[:, x, y, z + d, n], gsem.at[k, GD + d - SCATTER]))
            landed(own.at[:, x, y, :, n], gsem.at[k, G1 - SCATTER])
            landed(own.at[(slice(None), *xy(f, slice(None)), slice(None), n)], gsem.at[k, G2 - SCATTER])

        return dict(a=a, b=b, **hops(hop, forward), up=update, free=free, go=go, s=second, t=third, l=last), drain

    def z_colour():
        k, n = 2, rows[2]

        def hop(u, d):
            def side(sign, ref, kind, to):
                zj = z + sign * d
                if d < 3:
                    pl.when(z > 0 if sign > 0 else z < 3)(lambda: landed(ref.at[u, d], rsem.at[k, kind + d, u]))

                def body(i):
                    j = (u, i // 2, i % 2, zj, n)
                    own[j] = total([own[j], peer[j]] + ([ref[u, d, i // 2, i % 2]] if d < 3 else [])).astype(BF16)

                loop(4, body)
                send(own.at[u, :, :, zj, n], ref.at[u, d - 1], k, kind + d - 1, u, to)

            pl.when(z + d <= 3)(lambda: side(1, zuz, ZU, zu))
            pl.when(z - d >= 0)(lambda: side(-1, zdz, ZD, zd))

        def base(u, xj, yj):
            i = (u, xj, yj, z, n)
            return [own[i], peer[i], zuz[u, 0, xj, yj], zdz[u, 0, xj, yj]]

        def to_x(u):
            pl.when(z > 0)(lambda: landed(zuz.at[u, 0], rsem.at[k, ZU, u]))
            pl.when(z < 3)(lambda: landed(zdz.at[u, 0], rsem.at[k, ZD, u]))

            def body(i):
                own[u, 1 - x, i, z, n] = total(base(u, 1 - x, i)).astype(BF16)

            loop(2, body)
            send(own.at[u, 1 - x, :, z, n], r1z.at[u], k, S1, u, xn)

        def to_y(u):
            landed(r1z.at[u], rsem.at[k, S1, u])
            i = (u, x, 1 - y, z, n)
            own[i] = total(base(u, x, 1 - y) + [r1z[u, 1 - y]]).astype(BF16)
            send(own.at[i], r2z.at[u], k, S2, u, yn)

        def update(u):
            mat, h = u // HALVES, u % HALVES
            landed(r2z.at[u], rsem.at[k, S2, u])

            def body(i):
                p, q = pl.ds(row[k] + i * 16, 16), pl.ds(i * 16, 16)
                j = (u, x, y, z, p)
                g = total([own[j], peer[j], zuz[u, 0, x, y, q], zdz[u, 0, x, y, q], r1z[u, y, q], r2z[u, q]]).astype(BF16).astype(F32)
                i = (mat, h, p)
                own[j], mb[i], vb[i] = adamw(wb[i].astype(F32), mb[i], vb[i], g)

            loop(split[k] // 16, body)

        def free(u):
            for d in (1, 2, 3):
                pl.when(z + d <= 3)(lambda: landed(own.at[u, :, :, z + d, n], ssem.at[k, ZU + d - 1, u]))
                pl.when(z - d >= 0)(lambda: landed(own.at[u, :, :, z - d, n], ssem.at[k, ZD + d - 1, u]))
            landed(own.at[u, 1 - x, :, z, n], ssem.at[k, S1, u])
            landed(own.at[u, x, 1 - y, z, n], ssem.at[k, S2, u])
            give(k)

        def go(u):
            mine = own.at[u, x, y, z, n]
            take(k, Y)
            send(mine, mine, k, G1, u, yn)

        def second(u):
            landed(own.at[u, x, 1 - y, z, n], rsem.at[k, G1, u])
            ref = own.at[u, x, :, z, n]
            take(k, X)
            send(ref, ref, k, G2, u, xn)

        def third(u):
            landed(own.at[u, 1 - x, :, z, n], rsem.at[k, G2, u])
            ref = own.at[u, :, :, z, n]

            @pl.when(z < 3)
            def _():
                take(k, UP)
                send(ref, ref, k, GU, u, zu)

            @pl.when(z > 0)
            def _():
                take(k, DOWN)
                send(ref, ref, k, GD, u, zd)

        def forward(u, d):

            @pl.when(z - d >= 0)
            def _():
                ref = own.at[u, :, :, z - d, n]
                landed(ref, rsem.at[k, GU + d - 1, u])
                if d < 3:
                    pl.when(z < 3)(lambda: send(ref, ref, k, GU + d, u, zu))

            @pl.when(z + d <= 3)
            def _():
                ref = own.at[u, :, :, z + d, n]
                landed(ref, rsem.at[k, GD + d - 1, u])
                if d < 3:
                    pl.when(z > 0)(lambda: send(ref, ref, k, GD + d, u, zd))

        def last(u):
            ref = own.at[u, :, :, :, n]
            take(k, CORE)
            send(ref, peer.at[u, :, :, :, n], k, GP, u, cn)

        def drain():
            landed(own.at[:, x, y, z, n], gsem.at[k, G1 - SCATTER])
            landed(own.at[:, x, :, z, n], gsem.at[k, G2 - SCATTER])
            for d in (0, 1, 2):
                pl.when((z - d >= 0) & (z < 3))(lambda: landed(own.at[:, :, :, z - d, n], gsem.at[k, GU + d - SCATTER]))
                pl.when((z + d <= 3) & (z > 0))(lambda: landed(own.at[:, :, :, z + d, n], gsem.at[k, GD + d - SCATTER]))

        return dict(a=to_x, b=to_y, **hops(hop, forward), up=update, free=free, go=go, s=second, t=third, l=last), drain

    def arrive(u):
        landed(peer.at[u], psem.at[u])
        landed(own.at[u], osem.at[u])

        @pl.when(u == 1)
        def _():
            for copy in incoming:
                copy.wait()

    colours = [first_colours(0), first_colours(1), z_colour()]
    plan = [(lag, arrive if name == "arrive" else colours[k][0][name]) for lag, name, k in PLAN]

    @pl.loop(0, units + max(lag for lag, _ in plan))
    def _(t):
        for lag, stage in plan:
            u = t - lag
            pl.when((u >= 0) & (u < units))(functools.partial(stage, u))

    for k in range(3):

        @pl.loop(0, units)
        def _(u):
            landed(peer.at[u, :, :, :, rows[k]], rsem.at[k, GP, u])

        landed(own.at[:, :, :, :, rows[k]], gsem.at[k, GP - SCATTER])
        colours[k][1]()
    landed(peer, pssem.at[0])


def flush(*refs):
    own, peer, mb, vb, *whole = refs[:7]
    moments, sem = refs[7:13], refs[13]
    c = lax.axis_index("dp") % 2
    copies = []
    for u in range(own.shape[0]):
        mat, h = u // HALVES, u % HALVES
        copies.append((own.at[u], whole[mat // 2].at[mat % 2, :, :, :, c, h]))
        copies.append((peer.at[u], whole[mat // 2].at[mat % 2, :, :, :, 1 - c, h]))
    for a in range(3):
        copies.append((mb.at[pl.ds(2 * a, 2)], moments[a]))
        copies.append((vb.at[pl.ds(2 * a, 2)], moments[3 + a]))
    copies = [pltpu.make_async_copy(src, dst, sem.at[i]) for i, (src, dst) in enumerate(copies)]
    for copy in copies:
        copy.start()
    for copy in copies:
        copy.wait()


def call(terms, weights, m, v, split=SPLIT):
    mats, high = 2 * len(terms), sum(split)
    units = mats * HALVES
    rx, ry, rz = split
    block = [((mats, HALVES, high, 128), BF16)]
    for r in (rx, ry):
        block += [((units, 2, 4, r, 128), BF16), ((units, 4, r, 128), BF16)] + [((units, 3, r, 128), BF16)] * 2
    block += [((units, 2, rz, 128), BF16), ((units, rz, 128), BF16)] + [((units, 3, 2, 2, rz, 128), BF16)] * 2
    scratch = sum(math.prod(shape) * 2 for shape, _ in block)
    dma = pltpu.SemaphoreType.DMA
    half, moment = (units, 2, 2, 4, high, 128), (mats, HALVES, high, 128)
    held = pl.pallas_call(
        functools.partial(kernel, split, mats),
        out_shape=[pltpu.VMEM(half, BF16)] * 2 + [pltpu.VMEM(moment, F32)] * 2,
        in_specs=[pl.BlockSpec(memory_space=pltpu.HBM)] * 12,
        out_specs=[pl.BlockSpec(memory_space=pltpu.VMEM)] * 4,
        scratch_shapes=[pltpu.VMEM(*one) for one in block]
        + [dma((3, KINDS, units)), dma((3, SCATTER, units)), dma((3, KINDS - SCATTER)), dma((units,)), dma((units,)), dma((1,)), dma((9,))]
        + [pltpu.SemaphoreType.REGULAR((3, 5))],
        compiler_params=pltpu.CompilerParams(collective_id=0, has_side_effects=True, vmem_limit_bytes=scratch + (1 << 16)),
        name="step",
    )(*[pltpu.with_memory_space_constraint(one, pltpu.HBM) for one in (*terms, *weights, *m, *v)])
    some = jax.ShapeDtypeStruct
    return pl.pallas_call(
        flush,
        out_shape=[some((2, 2, 2, 4, 2, HALVES, high, 128), BF16)] * 3 + [some((2, HALVES, high, 128), F32)] * 6,
        in_specs=[pl.BlockSpec(memory_space=pltpu.VMEM)] * 4,
        out_specs=[pl.BlockSpec(memory_space=pltpu.HBM)] * 9,
        scratch_shapes=[dma((2 * units + 6,))],
        compiler_params=pltpu.CompilerParams(has_side_effects=True, vmem_limit_bytes=scratch + (1 << 16)),
        name="flush",
    )(*[pltpu.with_memory_space_constraint(one, pltpu.VMEM) for one in held])


def tiles(a):
    *lead, rows, columns = a.shape
    a = a.reshape(*lead, rows // 8, 8, columns // 128, 128)
    return jnp.swapaxes(a, -3, -2).reshape(*lead, rows * columns // 128, 128)


def untiles(a, rows, columns):
    lead = a.shape[:-2]
    a = a.reshape(*lead, rows // 8, columns // 128, 8, 128)
    return jnp.swapaxes(a, -3, -2).reshape(*lead, rows, columns)


def solution(mesh):
    def step(*arrays):
        terms, weights, m, v = (arrays[i : i + 3] for i in (0, 3, 6, 9))
        high = sum(SPLIT)
        out = call(
            [tiles(t[0]).reshape(2, 2, 2, 4, 2, HALVES, high, 128) for t in terms],
            [tiles(w).reshape(2, 32, HALVES, high, 128) for w in weights],
            [tiles(one).reshape(2, HALVES, high, 128) for one in m],
            [tiles(one).reshape(2, HALVES, high, 128) for one in v],
        )
        whole = [untiles(one.reshape(2, -1, 128), *w.shape[1:]) for one, w in zip(out, weights)]
        moments = [untiles(one.reshape(2, -1, 128), *old.shape[1:]) for one, old in zip(out[3:], (*m, *v), strict=True)]
        return (*whole, *moments)

    all_of, cut = P(None, None, None), P(None, "dp", None)
    return jax.shard_map(
        step,
        mesh=mesh,
        in_specs=(P(("rep", "dp"), None, None, None),) * 3 + (all_of,) * 3 + (cut,) * 6,
        out_specs=(P("rep", None, None),) * 3 + (P("rep", "dp", None),) * 6,
        check_vma=False,
    )
```

```python
import functools
import math

import jax
import jax.numpy as jnp
from jax import lax
from jax.experimental import pallas as pl
from jax.experimental.pallas import tpu as pltpu
from jax.sharding import PartitionSpec as P

MESH = pl.DeviceIdType.MESH
F32, BF16 = jnp.float32, jnp.bfloat16
SPLIT = (112, 128, 112)
HALVES = 2
PLAN = (
    (0, "arrive", 0),
    (5, "go", 2),
    (6, "f1", 0),
    (2, "b", 1),
    (2, "b", 0),
    (7, "s", 1),
    (8, "t", 0),
    (7, "t", 2),
    (4, "h2", 0),
    (4, "h2", 1),
    (1, "h2", 2),
    (5, "up", 0),
    (5, "free", 0),
    (3, "h3", 0),
    (10, "l", 2),
    (8, "t", 1),
    (6, "f2", 0),
    (6, "f2", 1),
    (5, "up", 1),
    (5, "go", 0),
    (5, "free", 1),
    (5, "go", 1),
    (0, "h3", 2),
    (3, "h3", 1),
    (10, "l", 1),
    (0, "a", 1),
    (9, "l", 0),
    (8, "f2", 2),
    (6, "f3", 0),
    (0, "a", 0),
    (7, "f1", 2),
    (6, "s", 0),
    (4, "h1", 0),
    (4, "h1", 1),
    (4, "up", 2),
    (4, "free", 2),
    (9, "f3", 2),
    (1, "h1", 2),
    (5, "s", 2),
    (3, "b", 2),
    (6, "f3", 1),
    (2, "a", 2),
    (5, "f1", 1),
)
S1, S2, ZU, ZD, GU, GD, G1, G2, GP = 0, 1, 2, 5, 8, 11, 14, 15, 16
SCATTER, KINDS = 8, 17
X, Y, UP, DOWN, CORE = range(5)


def adamw(w, m, v, g):
    m = 0.9 * m + 0.1 * g
    v = 0.95 * v + 0.05 * g * g
    step = m * lax.rsqrt(v + 1e-8) + 0.1 * w
    return (w - 0.02 * step).astype(BF16), m, v


def kernel(split, mats, *refs):
    (g0, g1, g2, w0, w1, w2, m0, m1, m2, v0, v1, v2, own, peer, mb, vb, *scratch) = refs
    wb, r1x, r2x, zux, zdx, r1y, r2y, zuy, zdy, r1z, r2z, zuz, zdz, *sems = scratch
    rsem, ssem, gsem, osem, psem, pssem, isem, credit = sems
    units = mats * HALVES
    row = (0, split[0], split[0] + split[1])
    rows = [pl.ds(row[k], split[k]) for k in range(3)]

    me = lax.axis_index("dp")
    c, z, y, x = me % 2, (me // 2) % 4, (me // 8) % 2, me // 16

    def at(x, y, z, c):
        return (0, ((x * 2 + y) * 4 + z) * 2 + c)

    xn, yn, zu, zd, cn = at(1 - x, y, z, c), at(x, 1 - y, z, c), at(x, y, z + 1, c), at(x, y, z - 1, c), at(x, y, z, 1 - c)

    def send(src, dst, k, kind, u, to, land=None):
        pltpu.make_async_remote_copy(
            src_ref=src,
            dst_ref=dst,
            send_sem=ssem.at[k, kind, u] if kind < SCATTER else gsem.at[k, kind - SCATTER],
            recv_sem=rsem.at[k, kind if land is None else land, u],
            device_id=to,
            device_id_type=MESH,
        ).start()

    def landed(ref, sem):
        pltpu.make_async_copy(ref, ref, sem).wait()

    def give(k):
        for side, to in ((X, xn), (Y, yn), (CORE, cn)):
            pl.semaphore_signal(credit.at[k, side], inc=1, device_id=to, device_id_type=MESH)
        pl.when(z < 3)(lambda: pl.semaphore_signal(credit.at[k, DOWN], inc=1, device_id=zu, device_id_type=MESH))
        pl.when(z > 0)(lambda: pl.semaphore_signal(credit.at[k, UP], inc=1, device_id=zd, device_id_type=MESH))

    def take(k, side):
        pl.semaphore_wait(credit.at[k, side], 1)

    barrier = pltpu.get_barrier_semaphore()
    for to in (xn, yn, cn):
        pl.semaphore_signal(barrier, inc=1, device_id=to, device_id_type=MESH)

    @pl.when(z < 3)
    def _():
        pl.semaphore_signal(barrier, inc=1, device_id=zu, device_id_type=MESH)

    @pl.when(z > 0)
    def _():
        pl.semaphore_signal(barrier, inc=1, device_id=zd, device_id_type=MESH)

    pl.semaphore_wait(barrier, 3 + jnp.where(z > 0, 1, 0) + jnp.where(z < 3, 1, 0))

    for u in range(units):
        mat, h = u // HALVES, u % HALVES
        g = (g0, g1, g2)[mat // 2]
        pltpu.make_async_remote_copy(
            src_ref=g.at[mat % 2, :, :, :, 1 - c, h],
            dst_ref=peer.at[u],
            send_sem=pssem.at[0],
            recv_sem=psem.at[u],
            device_id=cn,
            device_id_type=MESH,
        ).start()
        pltpu.make_async_copy(g.at[mat % 2, :, :, :, c, h], own.at[u], osem.at[u]).start()
    incoming = []
    for a in range(mats // 2):
        two = pl.ds(2 * a, 2)
        incoming.append(pltpu.make_async_copy((w0, w1, w2)[a].at[:, me], wb.at[two], isem.at[a]))
        incoming.append(pltpu.make_async_copy((m0, m1, m2)[a], mb.at[two], isem.at[3 + a]))
        incoming.append(pltpu.make_async_copy((v0, v1, v2)[a], vb.at[two], isem.at[6 + a]))
    for copy in incoming:
        copy.start()

    def blank(ref):
        @pl.loop(0, units)
        def _(u):
            ref[u] = jnp.zeros(ref.shape[1:], BF16)

    @pl.when(z == 0)
    def _():
        for ref in (zux, zuy, zuz):
            blank(ref)

    @pl.when(z == 3)
    def _():
        for ref in (zdx, zdy, zdz):
            blank(ref)

    def total(terms):
        acc = terms[0].astype(F32)
        for term in terms[1:]:
            acc = acc + term.astype(F32)
        return acc

    def loop(n, body):
        lax.fori_loop(0, n, lambda i, _: (body(i), 0)[1], 0)

    def hops(hop, forward):
        scatter = {f"h{d}": functools.partial(hop, d=d) for d in (1, 2, 3)}
        return scatter | {f"f{d}": functools.partial(forward, d=d) for d in (1, 2, 3)}

    def first_colours(k):
        f, s, fn, sn = ((x, y, xn, yn), (y, x, yn, xn))[k]
        first_side, second_side = ((X, Y), (Y, X))[k]
        r1, r2, up, down = ((r1x, r2x, zux, zdx), (r1y, r2y, zuy, zdy))[k]
        n = rows[k]

        def xy(one, two):
            return (one, two) if k == 0 else (two, one)

        def base(u, zj):
            i = (u, x, y, zj, n)
            return [own[i], peer[i], r1[u, s, zj], r2[u, zj]]

        def a(u):
            def body(i):
                j = (u, *xy(1 - f, i // 4), i % 4, n)
                own[j] = total([own[j], peer[j]]).astype(BF16)

            loop(8, body)
            send(own.at[(u, *xy(1 - f, slice(None)), slice(None), n)], r1.at[u], k, S1, u, fn)

        def b(u):
            landed(r1.at[u], rsem.at[k, S1, u])

            def body(i):
                j = (u, *xy(f, 1 - s), i, n)
                own[j] = total([own[j], peer[j], r1[u, 1 - s, i]]).astype(BF16)

            loop(4, body)
            send(own.at[(u, *xy(f, 1 - s), slice(None), n)], r2.at[u], k, S2, u, sn)

        def hop(u, d):
            if d == 3:
                landed(r2.at[u], rsem.at[k, S2, u])

            @pl.when(z + d <= 3)
            def _():
                if d < 3:
                    pl.when(z > 0)(lambda: landed(up.at[u, d], rsem.at[k, ZU + d, u]))
                i = (u, x, y, z + d, n)
                own[i] = total(base(u, z + d) + ([up[u, d]] if d < 3 else [])).astype(BF16)
                send(own.at[i], up.at[u, d - 1], k, ZU + d - 1, u, zu)

            @pl.when(z - d >= 0)
            def _():
                if d < 3:
                    pl.when(z < 3)(lambda: landed(down.at[u, d], rsem.at[k, ZD + d, u]))
                i = (u, x, y, z - d, n)
                own[i] = total(base(u, z - d) + ([down[u, d]] if d < 3 else [])).astype(BF16)
                send(own.at[i], down.at[u, d - 1], k, ZD + d - 1, u, zd)

        def update(u):
            mat, h = u // HALVES, u % HALVES
            pl.when(z > 0)(lambda: landed(up.at[u, 0], rsem.at[k, ZU, u]))
            pl.when(z < 3)(lambda: landed(down.at[u, 0], rsem.at[k, ZD, u]))

            def body(i):
                p, q = pl.ds(row[k] + i * 16, 16), pl.ds(i * 16, 16)
                j = (u, x, y, z, p)
                g = total([own[j], peer[j], r1[u, s, z, q], r2[u, z, q], up[u, 0, q], down[u, 0, q]]).astype(BF16).astype(F32)
                i = (mat, h, p)
                own[j], mb[i], vb[i] = adamw(wb[i].astype(F32), mb[i], vb[i], g)

            loop(split[k] // 16, body)

        def free(u):
            landed(own.at[(u, *xy(1 - f, slice(None)), slice(None), n)], ssem.at[k, S1, u])
            landed(own.at[(u, *xy(f, 1 - s), slice(None), n)], ssem.at[k, S2, u])
            for d in (1, 2, 3):
                pl.when(z + d <= 3)(lambda: landed(own.at[u, x, y, z + d, n], ssem.at[k, ZU + d - 1, u]))
                pl.when(z - d >= 0)(lambda: landed(own.at[u, x, y, z - d, n], ssem.at[k, ZD + d - 1, u]))
            give(k)

        def go(u):
            mine = own.at[u, x, y, z, n]

            @pl.when(z < 3)
            def _():
                take(k, UP)
                send(mine, mine, k, GU, u, zu)

            @pl.when(z > 0)
            def _():
                take(k, DOWN)
                send(mine, mine, k, GD, u, zd)

        def forward(u, d):

            @pl.when(z - d >= 0)
            def _():
                ref = own.at[u, x, y, z - d, n]
                landed(ref, rsem.at[k, GU + d - 1, u])
                if d < 3:
                    pl.when(z < 3)(lambda: send(ref, ref, k, GU + d, u, zu))

            @pl.when(z + d <= 3)
            def _():
                ref = own.at[u, x, y, z + d, n]
                landed(ref, rsem.at[k, GD + d - 1, u])
                if d < 3:
                    pl.when(z > 0)(lambda: send(ref, ref, k, GD + d, u, zd))

        def second(u):
            ref = own.at[u, x, y, :, n]
            take(k, second_side)
            send(ref, ref, k, G1, u, sn)

        def third(u):
            landed(own.at[(u, *xy(f, 1 - s), slice(None), n)], rsem.at[k, G1, u])
            ref = own.at[(u, *xy(f, slice(None)), slice(None), n)]
            take(k, first_side)
            send(ref, ref, k, G2, u, fn)

        def last(u):
            landed(own.at[(u, *xy(1 - f, slice(None)), slice(None), n)], rsem.at[k, G2, u])
            ref = own.at[u, :, :, :, n]
            take(k, CORE)
            send(ref, peer.at[u, :, :, :, n], k, GP, u, cn)

        def drain():
            for d in (0, 1, 2):
                pl.when((z - d >= 0) & (z < 3))(lambda: landed(own.at[:, x, y, z - d, n], gsem.at[k, GU + d - SCATTER]))
                pl.when((z + d <= 3) & (z > 0))(lambda: landed(own.at[:, x, y, z + d, n], gsem.at[k, GD + d - SCATTER]))
            landed(own.at[:, x, y, :, n], gsem.at[k, G1 - SCATTER])
            landed(own.at[(slice(None), *xy(f, slice(None)), slice(None), n)], gsem.at[k, G2 - SCATTER])

        return dict(a=a, b=b, **hops(hop, forward), up=update, free=free, go=go, s=second, t=third, l=last), drain

    def z_colour():
        k, n = 2, rows[2]

        def hop(u, d):
            def side(sign, ref, kind, to):
                zj = z + sign * d
                if d < 3:
                    pl.when(z > 0 if sign > 0 else z < 3)(lambda: landed(ref.at[u, d], rsem.at[k, kind + d, u]))

                def body(i):
                    j = (u, i // 2, i % 2, zj, n)
                    own[j] = total([own[j], peer[j]] + ([ref[u, d, i // 2, i % 2]] if d < 3 else [])).astype(BF16)

                loop(4, body)
                send(own.at[u, :, :, zj, n], ref.at[u, d - 1], k, kind + d - 1, u, to)

            pl.when(z + d <= 3)(lambda: side(1, zuz, ZU, zu))
            pl.when(z - d >= 0)(lambda: side(-1, zdz, ZD, zd))

        def base(u, xj, yj):
            i = (u, xj, yj, z, n)
            return [own[i], peer[i], zuz[u, 0, xj, yj], zdz[u, 0, xj, yj]]

        def to_x(u):
            pl.when(z > 0)(lambda: landed(zuz.at[u, 0], rsem.at[k, ZU, u]))
            pl.when(z < 3)(lambda: landed(zdz.at[u, 0], rsem.at[k, ZD, u]))

            def body(i):
                own[u, 1 - x, i, z, n] = total(base(u, 1 - x, i)).astype(BF16)

            loop(2, body)
            send(own.at[u, 1 - x, :, z, n], r1z.at[u], k, S1, u, xn)

        def to_y(u):
            landed(r1z.at[u], rsem.at[k, S1, u])
            i = (u, x, 1 - y, z, n)
            own[i] = total(base(u, x, 1 - y) + [r1z[u, 1 - y]]).astype(BF16)
            send(own.at[i], r2z.at[u], k, S2, u, yn)

        def update(u):
            mat, h = u // HALVES, u % HALVES
            landed(r2z.at[u], rsem.at[k, S2, u])

            def body(i):
                p, q = pl.ds(row[k] + i * 16, 16), pl.ds(i * 16, 16)
                j = (u, x, y, z, p)
                g = total([own[j], peer[j], zuz[u, 0, x, y, q], zdz[u, 0, x, y, q], r1z[u, y, q], r2z[u, q]]).astype(BF16).astype(F32)
                i = (mat, h, p)
                own[j], mb[i], vb[i] = adamw(wb[i].astype(F32), mb[i], vb[i], g)

            loop(split[k] // 16, body)

        def free(u):
            for d in (1, 2, 3):
                pl.when(z + d <= 3)(lambda: landed(own.at[u, :, :, z + d, n], ssem.at[k, ZU + d - 1, u]))
                pl.when(z - d >= 0)(lambda: landed(own.at[u, :, :, z - d, n], ssem.at[k, ZD + d - 1, u]))
            landed(own.at[u, 1 - x, :, z, n], ssem.at[k, S1, u])
            landed(own.at[u, x, 1 - y, z, n], ssem.at[k, S2, u])
            give(k)

        def go(u):
            mine = own.at[u, x, y, z, n]
            take(k, Y)
            send(mine, mine, k, G1, u, yn)

        def second(u):
            landed(own.at[u, x, 1 - y, z, n], rsem.at[k, G1, u])
            ref = own.at[u, x, :, z, n]
            take(k, X)
            send(ref, ref, k, G2, u, xn)

        def third(u):
            landed(own.at[u, 1 - x, :, z, n], rsem.at[k, G2, u])
            ref = own.at[u, :, :, z, n]

            @pl.when(z < 3)
            def _():
                take(k, UP)
                send(ref, ref, k, GU, u, zu)

            @pl.when(z > 0)
            def _():
                take(k, DOWN)
                send(ref, ref, k, GD, u, zd)

        def forward(u, d):

            @pl.when(z - d >= 0)
            def _():
                ref = own.at[u, :, :, z - d, n]
                landed(ref, rsem.at[k, GU + d - 1, u])
                if d < 3:
                    pl.when(z < 3)(lambda: send(ref, ref, k, GU + d, u, zu))

            @pl.when(z + d <= 3)
            def _():
                ref = own.at[u, :, :, z + d, n]
                landed(ref, rsem.at[k, GD + d - 1, u])
                if d < 3:
                    pl.when(z > 0)(lambda: send(ref, ref, k, GD + d, u, zd))

        def last(u):
            ref = own.at[u, :, :, :, n]
            take(k, CORE)
            send(ref, peer.at[u, :, :, :, n], k, GP, u, cn)

        def drain():
            landed(own.at[:, x, y, z, n], gsem.at[k, G1 - SCATTER])
            landed(own.at[:, x, :, z, n], gsem.at[k, G2 - SCATTER])
            for d in (0, 1, 2):
                pl.when((z - d >= 0) & (z < 3))(lambda: landed(own.at[:, :, :, z - d, n], gsem.at[k, GU + d - SCATTER]))
                pl.when((z + d <= 3) & (z > 0))(lambda: landed(own.at[:, :, :, z + d, n], gsem.at[k, GD + d - SCATTER]))

        return dict(a=to_x, b=to_y, **hops(hop, forward), up=update, free=free, go=go, s=second, t=third, l=last), drain

    def arrive(u):
        landed(peer.at[u], psem.at[u])
        landed(own.at[u], osem.at[u])

        @pl.when(u == 1)
        def _():
            for copy in incoming:
                copy.wait()

    colours = [first_colours(0), first_colours(1), z_colour()]
    plan = [(lag, arrive if name == "arrive" else colours[k][0][name]) for lag, name, k in PLAN]

    @pl.loop(0, units + max(lag for lag, _ in plan))
    def _(t):
        for lag, stage in plan:
            u = t - lag
            pl.when((u >= 0) & (u < units))(functools.partial(stage, u))

    for k in range(3):

        @pl.loop(0, units)
        def _(u):
            landed(peer.at[u, :, :, :, rows[k]], rsem.at[k, GP, u])

        landed(own.at[:, :, :, :, rows[k]], gsem.at[k, GP - SCATTER])
        colours[k][1]()
    landed(peer, pssem.at[0])


def flush(*refs):
    own, peer, mb, vb, *whole = refs[:7]
    moments, sem = refs[7:13], refs[13]
    c = lax.axis_index("dp") % 2
    copies = []
    for u in range(own.shape[0]):
        mat, h = u // HALVES, u % HALVES
        copies.append((own.at[u], whole[mat // 2].at[mat % 2, :, :, :, c, h]))
        copies.append((peer.at[u], whole[mat // 2].at[mat % 2, :, :, :, 1 - c, h]))
    for a in range(3):
        copies.append((mb.at[pl.ds(2 * a, 2)], moments[a]))
        copies.append((vb.at[pl.ds(2 * a, 2)], moments[3 + a]))
    copies = [pltpu.make_async_copy(src, dst, sem.at[i]) for i, (src, dst) in enumerate(copies)]
    for copy in copies:
        copy.start()
    for copy in copies:
        copy.wait()


def call(terms, weights, m, v, split=SPLIT):
    mats, high = 2 * len(terms), sum(split)
    units = mats * HALVES
    rx, ry, rz = split
    block = [((mats, HALVES, high, 128), BF16)]
    for r in (rx, ry):
        block += [((units, 2, 4, r, 128), BF16), ((units, 4, r, 128), BF16)] + [((units, 3, r, 128), BF16)] * 2
    block += [((units, 2, rz, 128), BF16), ((units, rz, 128), BF16)] + [((units, 3, 2, 2, rz, 128), BF16)] * 2
    scratch = sum(math.prod(shape) * 2 for shape, _ in block)
    dma = pltpu.SemaphoreType.DMA
    half, moment = (units, 2, 2, 4, high, 128), (mats, HALVES, high, 128)
    held = pl.pallas_call(
        functools.partial(kernel, split, mats),
        out_shape=[pltpu.VMEM(half, BF16)] * 2 + [pltpu.VMEM(moment, F32)] * 2,
        in_specs=[pl.BlockSpec(memory_space=pltpu.HBM)] * 12,
        out_specs=[pl.BlockSpec(memory_space=pltpu.VMEM)] * 4,
        scratch_shapes=[pltpu.VMEM(*one) for one in block]
        + [dma((3, KINDS, units)), dma((3, SCATTER, units)), dma((3, KINDS - SCATTER)), dma((units,)), dma((units,)), dma((1,)), dma((9,))]
        + [pltpu.SemaphoreType.REGULAR((3, 5))],
        compiler_params=pltpu.CompilerParams(collective_id=0, has_side_effects=True, vmem_limit_bytes=scratch + (1 << 16)),
        name="step",
    )(*[pltpu.with_memory_space_constraint(one, pltpu.HBM) for one in (*terms, *weights, *m, *v)])
    some = jax.ShapeDtypeStruct
    return pl.pallas_call(
        flush,
        out_shape=[some((2, 2, 2, 4, 2, HALVES, high, 128), BF16)] * 3 + [some((2, HALVES, high, 128), F32)] * 6,
        in_specs=[pl.BlockSpec(memory_space=pltpu.VMEM)] * 4,
        out_specs=[pl.BlockSpec(memory_space=pltpu.HBM)] * 9,
        scratch_shapes=[dma((2 * units + 6,))],
        compiler_params=pltpu.CompilerParams(has_side_effects=True, vmem_limit_bytes=scratch + (1 << 16)),
        name="flush",
    )(*[pltpu.with_memory_space_constraint(one, pltpu.VMEM) for one in held])


def tiles(a):
    *lead, rows, columns = a.shape
    a = a.reshape(*lead, rows // 8, 8, columns // 128, 128)
    return jnp.swapaxes(a, -3, -2).reshape(*lead, rows * columns // 128, 128)


def untiles(a, rows, columns):
    lead = a.shape[:-2]
    a = a.reshape(*lead, rows // 8, columns // 128, 8, 128)
    return jnp.swapaxes(a, -3, -2).reshape(*lead, rows, columns)


def solution(mesh):
    def step(*arrays):
        terms, weights, m, v = (arrays[i : i + 3] for i in (0, 3, 6, 9))
        high = sum(SPLIT)
        out = call(
            [tiles(t[0]).reshape(2, 2, 2, 4, 2, HALVES, high, 128) for t in terms],
            [tiles(w).reshape(2, 32, HALVES, high, 128) for w in weights],
            [tiles(one).reshape(2, HALVES, high, 128) for one in m],
            [tiles(one).reshape(2, HALVES, high, 128) for one in v],
        )
        whole = [untiles(one.reshape(2, -1, 128), *w.shape[1:]) for one, w in zip(out, weights)]
        moments = [untiles(one.reshape(2, -1, 128), *old.shape[1:]) for one, old in zip(out[3:], (*m, *v), strict=True)]
        return (*whole, *moments)

    all_of, cut = P(None, None, None), P(None, "dp", None)
    return jax.shard_map(
        step,
        mesh=mesh,
        in_specs=(P(("rep", "dp"), None, None, None),) * 3 + (all_of,) * 3 + (cut,) * 6,
        out_specs=(P("rep", None, None),) * 3 + (P("rep", "dp", None),) * 6,
        check_vma=False,
    )
```
